32 devices in a mesh: groups: 2 (over x), row: 16 (over z, y, core).
Axes of the slice: x: 2, y: 2, z: 4, core: 2. Of those that a mesh axis runs over, the one named last changes fastest.
Arguments:
- latent: bfloat16 [8, 16, 128, 16], P('groups', None, 'row'), parts along dimension 0, may hold values from -16 to 16, as said below
- w_in: bfloat16 [3, 3, 3, 16, 384], replicated, may hold values from -0.3125 to 0.3125
- gain_one: float32 [384], replicated, may hold values from 0.25 to 1.75
- w_mid: bfloat16 [3, 3, 3, 384, 384], replicated, may hold values from -0.0625 to 0.0625
- gain_two: float32 [384], replicated, may hold values from 0.25 to 1.75
- w_up: bfloat16 [3, 3, 384, 192], replicated, may hold values from -0.109375 to 0.109375
- gain_three: float32 [192], replicated, may hold values from 0.25 to 1.75
- w_low: bfloat16 [3, 3, 3, 192, 96], replicated, may hold values from -0.078125 to 0.078125
- gain_four: float32 [96], replicated, may hold values from 0.25 to 1.75
- w_out: bfloat16 [3, 3, 3, 96, 3], replicated, may hold values from -0.125 to 0.125
Outputs:
- frames_rgb: float32 [8, 3, 32, 256], P('groups', None, 'row'), parts along dimension 0
The draws below stay inside these ranges and needn't reach their ends.
There are 2 independent parts, one for each index of `groups`. The reference program is written for one: setup_inputs(seed, part) draws one part's arguments, and reference() takes and returns one part's arrays. A program takes and returns all parts, laid end to end along the dimension named above; an argument that names none is the same for every part. Nothing has to cross between parts.
Inputs may be any that keep to these rules, and one draw needn't show every extreme that they name: latent is real-valued.
All inputs are finite; a program needn't handle non-finite values.
Results may differ from the reference program's by a relative error of at most 0.0058.
Values may be sent and summed in bfloat16 or wider, within the bound.
A program may use at most 128 MiB of HBM per device.

```python
import math
import jax
import jax.numpy as jnp
from jax import lax

C_LAT = 16
C_HI = 384
C_MID = 192
C_LO = 96
FRAMES = 4
W = 128
H = 16


def draw_latent(key, part):
    keys = jax.random.split(jax.random.fold_in(key, 11), 5)
    shape = (FRAMES, H, W, C_LAT)
    frame_scale = jnp.exp(jax.random.uniform(keys[0], (FRAMES, 1, 1, C_LAT), jnp.float32, math.log(0.3), math.log(3.0)))
    row_scale = jnp.exp(jax.random.uniform(keys[1], (1, H, 1, 1), jnp.float32, math.log(0.4), math.log(2.5)))
    frame_shift = 0.7 * jax.random.normal(keys[2], (FRAMES, 1, 1, C_LAT), jnp.float32)
    row_shift = 0.7 * jax.random.normal(keys[3], (1, H, 1, C_LAT), jnp.float32)
    noise = jax.random.normal(keys[4], shape, jnp.float32)
    value = noise * frame_scale * row_scale + frame_shift + row_shift
    return jnp.clip(value, -16.0, 16.0).astype(jnp.bfloat16)


def scatter_about(key, shape, scale, limit, held_as=jnp.bfloat16):
    values = scale * jax.random.normal(key, shape, jnp.float32)
    return jnp.clip(values, min=-limit, max=limit).astype(held_as)


def setup_inputs(seed: int = 0, part: int = 0) -> dict:
    key_list = jax.random.split(jax.random.key(seed), 11)
    part_splits = jax.random.split(jax.random.fold_in(key_list[10], part), 11)
    latent = draw_latent(jax.random.fold_in(jax.random.fold_in(key_list[10], part), 71), part)
    w_in = scatter_about(key_list[1], (3, 3, 3, C_LAT, C_HI), (27 * C_LAT) ** -0.5, 0.3125)
    gain_one = jnp.clip(1.0 + 0.15 * jax.random.normal(key_list[2], (C_HI,), jnp.float32), 0.25, 1.75)
    w_mid = scatter_about(key_list[3], (3, 3, 3, C_HI, C_HI), (27 * C_HI) ** -0.5, 0.0625)
    gain_two = jnp.clip(1.0 + 0.15 * jax.random.normal(key_list[4], (C_HI,), jnp.float32), 0.25, 1.75)
    w_up = scatter_about(key_list[5], (3, 3, C_HI, C_MID), (9 * C_HI) ** -0.5, 0.109375)
    gain_three = jnp.clip(1.0 + 0.15 * jax.random.normal(key_list[6], (C_MID,), jnp.float32), 0.25, 1.75)
    w_low = scatter_about(key_list[7], (3, 3, 3, C_MID, C_LO), (27 * C_MID) ** -0.5, 0.078125)
    gain_four = jnp.clip(1.0 + 0.15 * jax.random.normal(key_list[8], (C_LO,), jnp.float32), 0.25, 1.75)
    w_out = scatter_about(key_list[9], (3, 3, 3, C_LO, 3), (27 * C_LO) ** -0.5, 0.125)
    return {"latent": latent, "w_in": w_in, "gain_one": gain_one, "w_mid": w_mid, "gain_two": gain_two, "w_up": w_up, "gain_three": gain_three, "w_low": w_low, "gain_four": gain_four, "w_out": w_out}


eps = 1e-06

def causal_conv(field, weight):
    frame_count, height, width, inner = field.shape
    padded = jnp.pad(field, ((2, 0), (1, 1), (1, 1), (0, 0)))
    total = jnp.zeros((frame_count * height * width, weight.shape[-1]), jnp.float32)
    for offset_t in range(3):
        for offset_h in range(3):
            for offset_w in range(3):
                window = padded[offset_t:offset_t + frame_count, offset_h:offset_h + height, offset_w:offset_w + width]
                total = total + jnp.dot(window.reshape(-1, inner), weight[offset_t, offset_h, offset_w], preferred_element_type=jnp.float32)
    return total.reshape(frame_count, height, width, -1)

def plane_conv(field, weight):
    frame_count, height, width, inner = field.shape
    padded = jnp.pad(field, ((0, 0), (1, 1), (1, 1), (0, 0)))
    total = jnp.zeros((frame_count * height * width, weight.shape[-1]), jnp.float32)
    for offset_h in range(3):
        for offset_w in range(3):
            window = padded[:, offset_h:offset_h + height, offset_w:offset_w + width]
            total = total + jnp.dot(window.reshape(-1, inner), weight[offset_h, offset_w], preferred_element_type=jnp.float32)
    return total.reshape(frame_count, height, width, -1)

def rms_act(field, gain):
    scale = lax.rsqrt(lax.optimization_barrier(jnp.mean(field * field, axis=-1, keepdims=True)) + eps)
    return jax.nn.silu(field * scale * gain).astype(jnp.bfloat16)

def reference(latent, w_in, gain_one, w_mid, gain_two, w_up, gain_three, w_low, gain_four, w_out):
    first = causal_conv(latent, w_in)
    act_one = rms_act(first, gain_one)
    second = first + causal_conv(act_one, w_mid)
    act_two = rms_act(second, gain_two)
    upsampled = jnp.repeat(jnp.repeat(act_two, 2, axis=1), 2, axis=2)
    third = plane_conv(upsampled, w_up)
    act_three = rms_act(third, gain_three)
    fourth = causal_conv(act_three, w_low)
    act_four = rms_act(fourth, gain_four)
    colour = causal_conv(act_four, w_out)
    return jnp.transpose(colour, (0, 3, 1, 2))
```

```python
import functools

import jax
import jax.numpy as jnp
from jax import lax
from jax.experimental import pallas as pl
from jax.experimental.pallas import tpu as pltpu
from jax.sharding import PartitionSpec as P

eps = 1e-06
f32, bf16 = jnp.float32, jnp.bfloat16


def silu(z):
    return z / (1.0 + jnp.exp(-z))


def rms_act(field, gain):
    mean = jnp.mean(field * field, axis=-1, keepdims=True)
    return silu(field * lax.rsqrt(mean + eps) * gain)


def pair_norm(field, gain, low):
    half = field.shape[-1] // 2
    square = field * field
    first = jnp.sum(jnp.where(low, square, 0.0), axis=-1, keepdims=True)
    second = jnp.sum(jnp.where(low, 0.0, square), axis=-1, keepdims=True)
    scale = jnp.where(low, lax.rsqrt(first / half + eps), lax.rsqrt(second / half + eps))
    return silu(field * scale * gain)


def dot(a, b):
    return jnp.dot(a, b, preferred_element_type=f32)


def kernel(
    sizes, devices,
    g_ref, g1_ref, g2_ref, g3_ref, g4_ref,
    win_hbm, wmid_hbm, wup_hbm, wlow_hbm, wout_ref,
    out_ref,
    win, wmid, wup, wlow,
    gs, a1, first_mid, b0, b1, sent, a3, a3s, ys, part, got,
    wsem, send_sem, recv_sem, psend, precv,
):
    frames, cols, c1, c2, c3, tall = sizes
    me = lax.axis_index("row")
    is_first, is_last = me == 0, me == devices - 1
    has_up, has_down = me > 0, me < devices - 1

    copies = [pltpu.make_async_copy(win_hbm, win, wsem.at[0])]
    for i, a in enumerate((2, 1, 0)):
        copies.append(pltpu.make_async_copy(wmid_hbm.at[a], wmid.at[a], wsem.at[1 + i]))
    copies.append(pltpu.make_async_copy(wup_hbm, wup, wsem.at[4]))
    copies.append(pltpu.make_async_copy(wlow_hbm, wlow, wsem.at[5]))
    for copy in copies:
        copy.start()

    barrier = pltpu.get_barrier_semaphore()

    @pl.when(has_up)
    def _():
        pl.semaphore_signal(barrier, inc=1, device_id={"row": me - 1}, device_id_type=pl.DeviceIdType.MESH)

    @pl.when(has_down)
    def _():
        pl.semaphore_signal(barrier, inc=1, device_id={"row": me + 1}, device_id_type=pl.DeviceIdType.MESH)

    pl.semaphore_wait(barrier, has_up.astype(jnp.int32) + has_down.astype(jnp.int32))

    for t in range(frames):
        b1[t, cols:tall, :] = jnp.zeros((tall - cols, 3 * c1), bf16)

    @pl.when(is_first)
    def _():
        for t in range(frames):
            b1[t, 0:cols, 0:c1] = jnp.zeros((cols, c1), bf16)
        got[0] = jnp.zeros(got.shape[1:], f32)

    @pl.when(is_last)
    def _():
        for t in range(frames):
            b1[t, 0:cols, 2 * c1 : 3 * c1] = jnp.zeros((cols, c1), bf16)
        got[1] = jnp.zeros(got.shape[1:], f32)

    row_id = lax.broadcasted_iota(jnp.int32, (cols, 1), 0)
    lanes = g_ref.shape[-1]
    for t in range(frames):
        g = g_ref[t].astype(f32)
        left = jnp.where(row_id == 0, 0.0, pltpu.roll(g, 1, 0))
        right = jnp.where(row_id == cols - 1, 0.0, pltpu.roll(g, cols - 1, 0))
        gs[t, :, 0:lanes] = left.astype(bf16)
        gs[t, :, lanes : 2 * lanes] = g.astype(bf16)
        gs[t, :, 2 * lanes : 3 * lanes] = right.astype(bf16)

    copies[0].wait()
    for b in range(3):
        keep = None if b == 1 else (has_up if b == 0 else has_down).astype(f32)
        for t in range(frames):
            total = None
            for a in range(3):
                s = t + a - 2
                if s >= 0:
                    d = dot(gs[s], win[a, :, b * c1 : (b + 1) * c1])
                    total = d if total is None else total + d
            if b == 1:
                first_mid[t] = total
            act = rms_act(total, g1_ref[...])
            if keep is not None:
                act = act * keep
            left = jnp.where(row_id == 0, 0.0, pltpu.roll(act, 1, 0))
            right = jnp.where(row_id == cols - 1, 0.0, pltpu.roll(act, cols - 1, 0))
            base = 3 * b * c1
            a1[t, :, base : base + c1] = left.astype(bf16)
            a1[t, :, base + c1 : base + 2 * c1] = act.astype(bf16)
            a1[t, :, base + 2 * c1 : base + 3 * c1] = right.astype(bf16)

    def halo(t, down):
        lane = 0 if down else 2 * c1
        peer = me + 1 if down else me - 1
        return pltpu.make_async_remote_copy(
            src_ref=sent.at[t],
            dst_ref=b1.at[t, pl.ds(0, cols), pl.ds(lane, c1)],
            send_sem=send_sem.at[int(down), t],
            recv_sem=recv_sem.at[int(down), t],
            device_id={"row": peer},
            device_id_type=pl.DeviceIdType.MESH,
        )

    waited = set()
    for t in range(frames):
        total = first_mid[t]
        for i, a in enumerate((2, 1, 0)):
            s = t + a - 2
            if s >= 0:
                if a not in waited:
                    waited.add(a)
                    copies[1 + i].wait()
                total = total + dot(a1[s], wmid[a])
        act = rms_act(total, g2_ref[...]).astype(bf16)
        sent[t] = act
        b1[t, 0:cols, c1 : 2 * c1] = act

        @pl.when(has_down)
        def _(t=t):
            halo(t, True).start()

        @pl.when(has_up)
        def _(t=t):
            halo(t, False).start()

    for i, a in enumerate((2, 1, 0)):
        if a not in waited:
            copies[1 + i].wait()
    copies[4].wait()
    copies[5].wait()

    lane3 = lax.broadcasted_iota(jnp.int32, (1, 2 * c2), 1)
    low3 = lane3 < c2
    tall_id = lax.broadcasted_iota(jnp.int32, (tall, 1), 0)
    keep_up, keep_down = has_up.astype(f32), has_down.astype(f32)
    lane4 = lax.broadcasted_iota(jnp.int32, (1, cols), 1)
    block = ys.shape[2] // 9

    def send_part(t, down):
        peer = me + 1 if down else me - 1
        return pltpu.make_async_remote_copy(
            src_ref=part.at[0 if down else 1, t],
            dst_ref=got.at[0 if down else 1, t],
            send_sem=psend.at[int(down), t],
            recv_sem=precv.at[int(down), t],
            device_id={"row": peer},
            device_id_type=pl.DeviceIdType.MESH,
        )

    for t in range(frames):
        @pl.when(has_up)
        def _(t=t):
            halo(t, True).wait_recv()

        @pl.when(has_down)
        def _(t=t):
            halo(t, False).wait_recv()

        b0[t] = pltpu.roll(b1[t].astype(f32), 1, 0).astype(bf16)
        for p in range(2):
            span = slice(p * c1, p * c1 + 2 * c1)
            third = dot(b0[t, :, span], wup[0]) + dot(b1[t, :, span], wup[1])
            for parity in range(2):
                field = third[:, parity * 2 * c2 : (parity + 1) * 2 * c2]
                act = pair_norm(field, g3_ref[...], low3)
                edge = keep_up if p == 0 else keep_down
                outer = low3 if p == 0 else jnp.logical_not(low3)
                act = act * jnp.where(outer, edge, 1.0)
                drop = 0 if parity == 0 else cols
                act = jnp.where(tall_id == drop, 0.0, act)
                base = parity * 4 * c2 + p * 2 * c2
                a3[t, :, base : base + 2 * c2] = act.astype(bf16)
                a3s[t, :, base : base + 2 * c2] = pltpu.roll(act, tall - 1, 0).astype(bf16)

        for parity in range(2):
            total = None
            for a in range(3):
                s = t + a - 2
                if s < 0:
                    continue
                if parity == 0:
                    d = dot(a3[s, 0:cols, :], wlow[a, 0 : 8 * c2, :])
                    d += dot(a3s[s, 0:cols, 0 : 4 * c2], wlow[a, 8 * c2 : 12 * c2, :])
                else:
                    d = dot(a3[s, 0:cols, 4 * c2 : 8 * c2], wlow[a, 0 : 4 * c2, :])
                    d += dot(a3s[s, 0:cols, :], wlow[a, 4 * c2 : 12 * c2, :])
                total = d if total is None else total + d
            acts = []
            half = total.shape[-1] // 2
            for q in range(2):
                field = total[:, q * half : (q + 1) * half]
                mean = jnp.sum(field * field, axis=-1, keepdims=True) / c3
                acts.append(silu(field * lax.rsqrt(mean + eps) * g4_ref[...]).astype(bf16))
            act = jnp.concatenate(acts, axis=-1)
            ys[t, parity] = lax.dot_general(
                wout_ref[...], act, (((1,), (1,)), ((), ())), preferred_element_type=f32
            )

        even, odd = None, None
        for a in range(3):
            s = t + a - 2
            if s < 0:
                continue
            taps = [[ys[s, parity, (3 * a + e) * block : (3 * a + e + 1) * block, :] for e in range(3)] for parity in range(2)]
            before = jnp.where(lane4 == 0, 0.0, pltpu.roll(taps[1][0], 1, 1))
            after = jnp.where(lane4 == cols - 1, 0.0, pltpu.roll(taps[0][2], cols - 1, 1))
            new_even = before + taps[0][1] + taps[1][2]
            new_odd = taps[0][0] + taps[1][1] + after
            even = new_even if even is None else even + new_even
            odd = new_odd if odd is None else odd + new_odd
        rows = block // 4
        for parity, value in enumerate((even, odd)):
            part[1, t, parity] = value[0:rows]
            part[0, t, parity] = value[3 * rows : 4 * rows]
            out_ref[t, parity] = value[rows : 3 * rows]

        @pl.when(has_down)
        def _(t=t):
            send_part(t, True).start()

        @pl.when(has_up)
        def _(t=t):
            send_part(t, False).start()

    for t in range(frames):
        @pl.when(has_up)
        def _(t=t):
            send_part(t, True).wait_recv()
            halo(t, False).wait_send()
            send_part(t, False).wait_send()

        @pl.when(has_down)
        def _(t=t):
            send_part(t, False).wait_recv()
            halo(t, True).wait_send()
            send_part(t, True).wait_send()

        rows = block // 4
        for parity in range(2):
            out_ref[t, parity, 0:rows] += got[0, t, parity]
            out_ref[t, parity, rows : 2 * rows] += got[1, t, parity]


def per_device(latent, w_in, gain_one, w_mid, gain_two, w_up, gain_three, w_low, gain_four, w_out):
    frames, height, tw, c0 = latent.shape
    devices = lax.axis_size("row")
    cols = tw * devices
    assert height == devices
    c1, c2, c3 = w_in.shape[-1], w_up.shape[-1], w_low.shape[-1]
    colours = w_out.shape[-1]
    tall = cols + 16
    half, rows = 128, 8

    padded = jnp.pad(latent, ((0, 0), (2, 2), (0, 0), (0, 0)))
    stacked = jnp.stack([padded[:, s : s + height] for s in range(5)], axis=3)
    blocks = jnp.transpose(stacked, (1, 0, 2, 3, 4)).reshape(height, frames, tw, 5 * c0)
    arrived = lax.all_to_all(blocks, "row", split_axis=0, concat_axis=0, tiled=True)
    g = jnp.transpose(arrived, (1, 0, 2, 3)).reshape(frames, cols, 5 * c0)
    lanes = -(-5 * c0 // 128) * 128
    g = jnp.pad(g, ((0, 0), (0, 0), (0, lanes - 5 * c0)))

    tap = jnp.transpose(w_in, (0, 2, 1, 3, 4)).reshape(3, 3, 3 * c0, c1)
    win = jnp.concatenate(
        [jnp.pad(tap, ((0, 0), (0, 0), (b * c0, lanes - (3 + b) * c0), (0, 0))) for b in range(3)], axis=-1
    ).reshape(3, 3 * lanes, 3 * c1)
    wmid = w_mid.reshape(3, 9 * c1, c1)

    wide = w_up.astype(f32)

    def fold(w, axis):
        k0, k1, k2 = (lax.index_in_dim(w, i, axis, keepdims=False) for i in range(3))
        return ((k0 + k1, k0), (k2, k1 + k2))

    folded = []
    by_row = fold(wide, 0)
    for in_col in range(2):
        in_rows = []
        for in_row in range(2):
            outs = [fold(by_row[in_row][out_row], 0)[in_col][parity] for parity in range(2) for out_row in range(2)]
            in_rows.append(jnp.concatenate(outs, axis=-1))
        folded.append(jnp.concatenate(in_rows, axis=0))
    wup = jnp.stack(folded).astype(bf16)

    tap = jnp.transpose(w_low, (0, 2, 1, 3, 4)).reshape(3, 3, 3 * c2, c3)
    tap = jnp.pad(tap, ((0, 0), (0, 0), (0, 0), (0, half - c3)))
    wlow = jnp.concatenate(
        [jnp.pad(tap, ((0, 0), (0, 0), (q * c2, (1 - q) * c2), (0, 0))) for q in range(2)], axis=-1
    ).reshape(3, 12 * c2, 2 * half)

    tap = jnp.transpose(w_out, (0, 2, 1, 4, 3))
    tap = jnp.pad(tap, ((0, 0), (0, 0), (0, 0), (0, rows - colours), (0, half - c3)))
    zero = jnp.zeros((3, 3, rows, half), bf16)
    by_slot = []
    for slot in range(4):
        sides = []
        for q in range(2):
            b = q - slot + 2
            sides.append(tap[:, :, b] if 0 <= b <= 2 else zero)
        by_slot.append(jnp.concatenate(sides, axis=-1))
    wout = jnp.stack(by_slot, axis=2).reshape(9 * 4 * rows, 2 * half)

    gain_pair = jnp.concatenate([gain_three, gain_three]).reshape(1, 2 * c2)
    gain_last = jnp.pad(gain_four, (0, half - c3)).reshape(1, half)

    vmem = pl.BlockSpec(memory_space=pltpu.VMEM)
    any_space = pl.BlockSpec(memory_space=pl.ANY)
    out = pl.pallas_call(
        functools.partial(kernel, (frames, cols, c1, c2, c3, tall), devices),
        out_shape=jax.ShapeDtypeStruct((frames, 2, 2 * rows, cols), f32),
        in_specs=[vmem] * 5 + [any_space] * 4 + [vmem],
        out_specs=vmem,
        scratch_shapes=[
            pltpu.VMEM(win.shape, bf16),
            pltpu.VMEM(wmid.shape, bf16),
            pltpu.VMEM(wup.shape, bf16),
            pltpu.VMEM(wlow.shape, bf16),
            pltpu.VMEM((frames, cols, 3 * lanes), bf16),
            pltpu.VMEM((frames, cols, 9 * c1), bf16),
            pltpu.VMEM((frames, cols, c1), f32),
            pltpu.VMEM((frames, tall, 3 * c1), bf16),
            pltpu.VMEM((frames, tall, 3 * c1), bf16),
            pltpu.VMEM((frames, cols, c1), bf16),
            pltpu.VMEM((frames, tall, 8 * c2), bf16),
            pltpu.VMEM((frames, tall, 8 * c2), bf16),
            pltpu.VMEM((frames, 2, 9 * 4 * rows, cols), f32),
            pltpu.VMEM((2, frames, 2, rows, cols), f32),
            pltpu.VMEM((2, frames, 2, rows, cols), f32),
            pltpu.SemaphoreType.DMA((6,)),
            pltpu.SemaphoreType.DMA((2, frames)),
            pltpu.SemaphoreType.DMA((2, frames)),
            pltpu.SemaphoreType.DMA((2, frames)),
            pltpu.SemaphoreType.DMA((2, frames)),
        ],
        compiler_params=pltpu.CompilerParams(
            collective_id=0, has_side_effects=True, vmem_limit_bytes=60 * 1024 * 1024
        ),
    )(
        g, gain_one.reshape(1, c1), gain_two.reshape(1, c1), gain_pair, gain_last,
        win, wmid, wup, wlow, wout,
    )
    out = out.reshape(frames, 2, 2, rows, cols)[:, :, :, :colours]
    return jnp.transpose(out, (0, 3, 2, 4, 1)).reshape(frames, colours, 2, 2 * cols)


def solution(mesh):
    placed = (P("groups", None, "row", None), P(), P(), P(), P(), P(), P(), P(), P(), P())
    return jax.shard_map(
        per_device,
        mesh=mesh,
        in_specs=placed,
        out_specs=P("groups", None, "row", None),
        check_vma=False,
    )
```

```python
import functools

import jax
import jax.numpy as jnp
from jax import lax
from jax.experimental import pallas as pl
from jax.experimental.pallas import tpu as pltpu
from jax.sharding import PartitionSpec as P

eps = 1e-06
f32, bf16 = jnp.float32, jnp.bfloat16


def silu(z):
    return z / (1.0 + jnp.exp(-z))


def rms_act(field, gain):
    mean = jnp.mean(field * field, axis=-1, keepdims=True)
    return silu(field * lax.rsqrt(mean + eps) * gain)


def pair_norm(field, gain, low):
    half = field.shape[-1] // 2
    square = field * field
    first = jnp.sum(jnp.where(low, square, 0.0), axis=-1, keepdims=True)
    second = jnp.sum(jnp.where(low, 0.0, square), axis=-1, keepdims=True)
    scale = jnp.where(low, lax.rsqrt(first / half + eps), lax.rsqrt(second / half + eps))
    return silu(field * scale * gain)


def dot(a, b):
    return jnp.dot(a, b, preferred_element_type=f32)


def dot_t(a, b):
    return lax.dot_general(a, b, (((1,), (1,)), ((), ())), preferred_element_type=f32)


def kernel(
    sizes, devices,
    g_ref, gains_ref,
    win_hbm, wmid_hbm, wup_hbm, wlow_hbm, wout_ref,
    out_ref,
    raw_in, raw_up, raw_low,
    win, wmid, wup, wlow,
    gs, a1, first_mid, b0, b1, sent, a3, a3s, ys, part, got,
    wsem, send_sem, recv_sem, psend, precv,
):
    frames, cols, c0, c1, c2, c3, tall = sizes
    g1, g2 = gains_ref[0:1, 0:c1], gains_ref[1:2, 0:c1]
    g3, g4 = gains_ref[2:3, 0 : 2 * c2], gains_ref[3:4, 0 : wlow.shape[-1] // 2]
    me = lax.axis_index("row")
    is_first, is_last = me == 0, me == devices - 1
    has_up, has_down = me > 0, me < devices - 1

    copies = [pltpu.make_async_copy(win_hbm, raw_in, wsem.at[0])]
    copies.append(pltpu.make_async_copy(wup_hbm, raw_up, wsem.at[4]))
    copies.append(pltpu.make_async_copy(wlow_hbm, raw_low, wsem.at[5]))
    for i, a in enumerate((2, 1, 0)):
        copies.append(pltpu.make_async_copy(wmid_hbm.at[a], wmid.at[a], wsem.at[1 + i]))
    for copy in copies:
        copy.start()

    barrier = pltpu.get_barrier_semaphore()

    @pl.when(has_up)
    def _():
        pl.semaphore_signal(barrier, inc=1, device_id={"row": me - 1}, device_id_type=pl.DeviceIdType.MESH)

    @pl.when(has_down)
    def _():
        pl.semaphore_signal(barrier, inc=1, device_id={"row": me + 1}, device_id_type=pl.DeviceIdType.MESH)

    pl.semaphore_wait(barrier, has_up.astype(jnp.int32) + has_down.astype(jnp.int32))

    for t in range(frames):
        b1[t, cols:tall, :] = jnp.zeros((tall - cols, 3 * c1), bf16)

    @pl.when(is_first)
    def _():
        for t in range(frames):
            b1[t, 0:cols, 0:c1] = jnp.zeros((cols, c1), bf16)
        got[0] = jnp.zeros(got.shape[1:], f32)

    @pl.when(is_last)
    def _():
        for t in range(frames):
            b1[t, 0:cols, 2 * c1 : 3 * c1] = jnp.zeros((cols, c1), bf16)
        got[1] = jnp.zeros(got.shape[1:], f32)

    row_id = lax.broadcasted_iota(jnp.int32, (cols, 1), 0)
    lanes = g_ref.shape[-1]
    for t in range(frames):
        g = g_ref[t].astype(f32)
        left = jnp.where(row_id == 0, 0.0, pltpu.roll(g, 1, 0))
        right = jnp.where(row_id == cols - 1, 0.0, pltpu.roll(g, cols - 1, 0))
        gs[t, :, 0:lanes] = left.astype(bf16)
        gs[t, :, lanes : 2 * lanes] = g.astype(bf16)
        gs[t, :, 2 * lanes : 3 * lanes] = right.astype(bf16)

    for a in range(3):
        win[a] = jnp.zeros(win.shape[1:], bf16)
    copies[0].wait()
    for a in range(3):
        for e in range(3):
            for b in range(3):
                block = raw_in[a, b, e]
                for slot in range(3):
                    at = e * lanes + (slot + b) * c0
                    win[a, at : at + c0, slot * c1 : (slot + 1) * c1] = block

    copies[1].wait()
    for slot in range(2):
        for in_row in range(2):
            mixed = []
            for e in range(3):
                if slot == 0:
                    taps = (0, 1) if in_row == 0 else (2,)
                else:
                    taps = (0,) if in_row == 0 else (1, 2)
                value = raw_up[taps[0], e].astype(f32)
                for b in taps[1:]:
                    value = value + raw_up[b, e].astype(f32)
                mixed.append(value)
            k0, k1, k2 = mixed
            for parity in range(2):
                pair = (k0 + k1, k2) if parity == 0 else (k0, k1 + k2)
                at = parity * 2 * c2 + slot * c2
                for in_col in range(2):
                    wup[in_col, at : at + c2, in_row * c1 : (in_row + 1) * c1] = pair[in_col].astype(bf16)

    for a in range(3):
        wlow[a] = jnp.zeros(wlow.shape[1:], bf16)
    copies[2].wait()
    for a in range(3):
        for e in range(3):
            for b in range(3):
                block = raw_low[a, b, e]
                for q in range(2):
                    at = (4 * e + q + b) * c2
                    lane = q * (wlow.shape[-1] // 2)
                    wlow[a, at : at + c2, lane : lane + c3] = block

    for b in range(3):
        keep = None if b == 1 else (has_up if b == 0 else has_down).astype(f32)
        for t in range(frames):
            total = None
            for a in range(3):
                s = t + a - 2
                if s >= 0:
                    d = dot(gs[s], win[a, :, b * c1 : (b + 1) * c1])
                    total = d if total is None else total + d
            if b == 1:
                first_mid[t] = total
            act = rms_act(total, g1)
            if keep is not None:
                act = act * keep
            left = jnp.where(row_id == 0, 0.0, pltpu.roll(act, 1, 0))
            right = jnp.where(row_id == cols - 1, 0.0, pltpu.roll(act, cols - 1, 0))
            base = 3 * b * c1
            a1[t, :, base : base + c1] = left.astype(bf16)
            a1[t, :, base + c1 : base + 2 * c1] = act.astype(bf16)
            a1[t, :, base + 2 * c1 : base + 3 * c1] = right.astype(bf16)

    def halo(t, down):
        lane = 0 if down else 2 * c1
        peer = me + 1 if down else me - 1
        return pltpu.make_async_remote_copy(
            src_ref=sent.at[t],
            dst_ref=b1.at[t, pl.ds(0, cols), pl.ds(lane, c1)],
            send_sem=send_sem.at[int(down), t],
            recv_sem=recv_sem.at[int(down), t],
            device_id={"row": peer},
            device_id_type=pl.DeviceIdType.MESH,
        )

    waited = set()
    for t in range(frames):
        total = first_mid[t]
        for i, a in enumerate((2, 1, 0)):
            s = t + a - 2
            if s >= 0:
                if a not in waited:
                    waited.add(a)
                    copies[3 + i].wait()
                total = total + dot(a1[s], wmid[a])
        act = rms_act(total, g2).astype(bf16)
        sent[t] = act
        b1[t, 0:cols, c1 : 2 * c1] = act

        @pl.when(has_down)
        def _(t=t):
            halo(t, True).start()

        @pl.when(has_up)
        def _(t=t):
            halo(t, False).start()

    for i, a in enumerate((2, 1, 0)):
        if a not in waited:
            copies[3 + i].wait()

    lane3 = lax.broadcasted_iota(jnp.int32, (1, 2 * c2), 1)
    low3 = lane3 < c2
    tall_id = lax.broadcasted_iota(jnp.int32, (tall, 1), 0)
    keep_up, keep_down = has_up.astype(f32), has_down.astype(f32)
    lane4 = lax.broadcasted_iota(jnp.int32, (1, cols), 1)
    block = ys.shape[2] // 9

    def send_part(t, down):
        peer = me + 1 if down else me - 1
        return pltpu.make_async_remote_copy(
            src_ref=part.at[0 if down else 1, t],
            dst_ref=got.at[0 if down else 1, t],
            send_sem=psend.at[int(down), t],
            recv_sem=precv.at[int(down), t],
            device_id={"row": peer},
            device_id_type=pl.DeviceIdType.MESH,
        )

    for t in range(frames):
        @pl.when(has_up)
        def _(t=t):
            halo(t, True).wait_recv()

        @pl.when(has_down)
        def _(t=t):
            halo(t, False).wait_recv()

        b0[t] = pltpu.roll(b1[t].astype(f32), 1, 0).astype(bf16)
        for p in range(2):
            span = slice(p * c1, p * c1 + 2 * c1)
            third = dot_t(b0[t, :, span], wup[0]) + dot_t(b1[t, :, span], wup[1])
            for parity in range(2):
                field = third[:, parity * 2 * c2 : (parity + 1) * 2 * c2]
                act = pair_norm(field, g3, low3)
                edge = keep_up if p == 0 else keep_down
                outer = low3 if p == 0 else jnp.logical_not(low3)
                act = act * jnp.where(outer, edge, 1.0)
                drop = 0 if parity == 0 else cols
                act = jnp.where(tall_id == drop, 0.0, act)
                base = parity * 4 * c2 + p * 2 * c2
                a3[t, :, base : base + 2 * c2] = act.astype(bf16)
                a3s[t, :, base : base + 2 * c2] = pltpu.roll(act, tall - 1, 0).astype(bf16)

        for parity in range(2):
            total = None
            for a in range(3):
                s = t + a - 2
                if s < 0:
                    continue
                if parity == 0:
                    d = dot(a3[s, 0:cols, :], wlow[a, 0 : 8 * c2, :])
                    d += dot(a3s[s, 0:cols, 0 : 4 * c2], wlow[a, 8 * c2 : 12 * c2, :])
                else:
                    d = dot(a3[s, 0:cols, 4 * c2 : 8 * c2], wlow[a, 0 : 4 * c2, :])
                    d += dot(a3s[s, 0:cols, :], wlow[a, 4 * c2 : 12 * c2, :])
                total = d if total is None else total + d
            acts = []
            half = total.shape[-1] // 2
            for q in range(2):
                field = total[:, q * half : (q + 1) * half]
                mean = jnp.sum(field * field, axis=-1, keepdims=True) / c3
                acts.append(silu(field * lax.rsqrt(mean + eps) * g4).astype(bf16))
            act = jnp.concatenate(acts, axis=-1)
            ys[t, parity] = lax.dot_general(
                wout_ref[...], act, (((1,), (1,)), ((), ())), preferred_element_type=f32
            )

        even, odd = None, None
        for a in range(3):
            s = t + a - 2
            if s < 0:
                continue
            taps = [[ys[s, parity, (3 * a + e) * block : (3 * a + e + 1) * block, :] for e in range(3)] for parity in range(2)]
            before = jnp.where(lane4 == 0, 0.0, pltpu.roll(taps[1][0], 1, 1))
            after = jnp.where(lane4 == cols - 1, 0.0, pltpu.roll(taps[0][2], cols - 1, 1))
            new_even = before + taps[0][1] + taps[1][2]
            new_odd = taps[0][0] + taps[1][1] + after
            even = new_even if even is None else even + new_even
            odd = new_odd if odd is None else odd + new_odd
        rows = block // 4
        for parity, value in enumerate((even, odd)):
            part[1, t, parity] = value[0:rows]
            part[0, t, parity] = value[3 * rows : 4 * rows]
            out_ref[t, parity] = value[rows : 3 * rows]

        @pl.when(has_down)
        def _(t=t):
            send_part(t, True).start()

        @pl.when(has_up)
        def _(t=t):
            send_part(t, False).start()

    for t in range(frames):
        @pl.when(has_up)
        def _(t=t):
            send_part(t, True).wait_recv()
            halo(t, False).wait_send()
            send_part(t, False).wait_send()

        @pl.when(has_down)
        def _(t=t):
            send_part(t, False).wait_recv()
            halo(t, True).wait_send()
            send_part(t, True).wait_send()

        rows = block // 4
        for parity in range(2):
            out_ref[t, parity, 0:rows] += got[0, t, parity]
            out_ref[t, parity, rows : 2 * rows] += got[1, t, parity]


def per_device(latent, w_in, gain_one, w_mid, gain_two, w_up, gain_three, w_low, gain_four, w_out):
    frames, height, tw, c0 = latent.shape
    devices = lax.axis_size("row")
    cols = tw * devices
    assert height == devices
    c1, c2, c3 = w_in.shape[-1], w_up.shape[-1], w_low.shape[-1]
    colours = w_out.shape[-1]
    tall = cols + 16
    half, rows = 128, 8

    flat = jnp.transpose(latent, (1, 0, 2, 3)).reshape(height, frames, tw * c0)
    padded = jnp.pad(flat, ((2, 2), (0, 0), (0, 0)))
    blocks = jnp.stack([padded[s : s + height] for s in range(5)], axis=1)
    arrived = lax.all_to_all(blocks, "row", split_axis=0, concat_axis=0, tiled=True)
    g = arrived.reshape(devices, 5, frames, tw, c0)
    g = jnp.transpose(g, (2, 0, 3, 1, 4)).reshape(frames, cols, 5 * c0)
    lanes = -(-5 * c0 // 128) * 128
    g = jnp.pad(g, ((0, 0), (0, 0), (0, lanes - 5 * c0)))

    wmid = w_mid.reshape(3, 9 * c1, c1)
    wup = jnp.transpose(w_up, (0, 1, 3, 2))

    tap = jnp.transpose(w_out, (0, 2, 1, 4, 3))
    tap = jnp.pad(tap, ((0, 0), (0, 0), (0, 0), (0, rows - colours), (0, half - c3)))
    zero = jnp.zeros((3, 3, rows, half), bf16)
    by_slot = []
    for slot in range(4):
        sides = []
        for q in range(2):
            b = q - slot + 2
            sides.append(tap[:, :, b] if 0 <= b <= 2 else zero)
        by_slot.append(jnp.concatenate(sides, axis=-1))
    wout = jnp.stack(by_slot, axis=2).reshape(9 * 4 * rows, 2 * half)

    longest = max(c1, 2 * c2)
    gain_rows = (gain_one, gain_two, jnp.concatenate([gain_three, gain_three]), gain_four)
    gains = jnp.stack([jnp.pad(v, (0, longest - v.shape[0])) for v in gain_rows])

    vmem = pl.BlockSpec(memory_space=pltpu.VMEM)
    any_space = pl.BlockSpec(memory_space=pl.ANY)
    out = pl.pallas_call(
        functools.partial(kernel, (frames, cols, c0, c1, c2, c3, tall), devices),
        out_shape=jax.ShapeDtypeStruct((frames, 2, 2 * rows, cols), f32),
        in_specs=[vmem] * 2 + [any_space] * 4 + [vmem],
        out_specs=vmem,
        scratch_shapes=[
            pltpu.VMEM(w_in.shape, bf16),
            pltpu.VMEM(wup.shape, bf16),
            pltpu.VMEM(w_low.shape, bf16),
            pltpu.VMEM((3, 3 * lanes, 3 * c1), bf16),
            pltpu.VMEM(wmid.shape, bf16),
            pltpu.VMEM((2, 4 * c2, 2 * c1), bf16),
            pltpu.VMEM((3, 12 * c2, 2 * half), bf16),
            pltpu.VMEM((frames, cols, 3 * lanes), bf16),
            pltpu.VMEM((frames, cols, 9 * c1), bf16),
            pltpu.VMEM((frames, cols, c1), f32),
            pltpu.VMEM((frames, tall, 3 * c1), bf16),
            pltpu.VMEM((frames, tall, 3 * c1), bf16),
            pltpu.VMEM((frames, cols, c1), bf16),
            pltpu.VMEM((frames, tall, 8 * c2), bf16),
            pltpu.VMEM((frames, tall, 8 * c2), bf16),
            pltpu.VMEM((frames, 2, 9 * 4 * rows, cols), f32),
            pltpu.VMEM((2, frames, 2, rows, cols), f32),
            pltpu.VMEM((2, frames, 2, rows, cols), f32),
            pltpu.SemaphoreType.DMA((6,)),
            pltpu.SemaphoreType.DMA((2, frames)),
            pltpu.SemaphoreType.DMA((2, frames)),
            pltpu.SemaphoreType.DMA((2, frames)),
            pltpu.SemaphoreType.DMA((2, frames)),
        ],
        compiler_params=pltpu.CompilerParams(
            collective_id=0, has_side_effects=True, vmem_limit_bytes=60 * 1024 * 1024
        ),
    )(
        g, gains, w_in, wmid, wup, w_low, wout,
    )
    out = out.reshape(frames, 2, 2, rows, cols)[:, :, :, :colours]
    return jnp.transpose(out, (0, 3, 2, 4, 1)).reshape(frames, colours, 2, 2 * cols)


def solution(mesh):
    placed = (P("groups", None, "row", None), P(), P(), P(), P(), P(), P(), P(), P(), P())
    return jax.shard_map(
        per_device,
        mesh=mesh,
        in_specs=placed,
        out_specs=P("groups", None, "row", None),
        check_vma=False,
    )
```
